256 devices in a mesh: seq: 128 (over y, x_lo, z, core), dp: 2 (over x_hi).
Axes of the slice: x: 4 (x_hi: 2, x_lo: 2; x = x_hi * 2 + x_lo), y: 4, z: 8, core: 2. Of those that a mesh axis runs over, the one named last changes fastest.
Arguments:
- q_student: bfloat16 [2, 65536, 1536], P('dp', 'seq'), may hold values from -8 to 8
- kv_student: bfloat16 [2, 1024, 3072], P('dp', 'seq'), may hold values from -8 to 8
- q_target: bfloat16 [2, 65536, 1536], P('dp', 'seq'), may hold values from -8 to 8
- kv_target: bfloat16 [2, 1024, 3072], P('dp', 'seq'), may hold values from -8 to 8
Outputs:
- student_out: bfloat16 [2, 65536, 1536], P('dp', 'seq')
- target_out: bfloat16 [2, 65536, 1536], P('dp', 'seq')
- distill_loss: float32 [], replicated
The draws below stay inside these ranges and needn't reach their ends.
All inputs are finite; a program needn't handle non-finite values.
Results may differ from the reference program's by a relative error of at most 0.004.
Values may be sent and summed in bfloat16 or wider, within the bound.
No kernel may reach another device: no remote copies, remote signals or barrier semaphores. Data moves between devices by JAX's collectives and lax.ppermute only.
A program may use at most 128 MiB of HBM per device.

```python
import jax
import jax.numpy as jnp
from jax import lax

HEADS = 12
HD = 128
TOK_DEV = 512
TOKENS = 65536
KV_TOKENS = 1024
CLIPS = 2
N_SEQ = 128


def draw_pairs(key, value_growth):
    feature_width = HEADS * HD
    key_list = jax.random.split(key, 7)
    clip_frac = jnp.arange(CLIPS).astype(jnp.float32)
    value_scale = 1.0 + value_growth * 1.5 * clip_frac
    queries = jnp.clip(2.5 * jax.random.normal(key_list[0], (CLIPS, TOKENS, feature_width), jnp.float32), -8.0, 8.0)
    key_part = jnp.clip(jax.random.normal(key_list[1], (CLIPS, KV_TOKENS, feature_width), jnp.float32), -6.0, 6.0)
    value_part = jnp.clip(jax.random.normal(key_list[6], (CLIPS, KV_TOKENS, feature_width), jnp.float32) * value_scale[:, None, None], -8.0, 8.0)
    key_values = jnp.concatenate([key_part, value_part], axis=2)
    return (queries, key_values)


def draw_q_student(key, part):
    return draw_pairs(jax.random.fold_in(key, 11), 0.0)[0].astype(jnp.bfloat16)


def draw_kv_student(key, part):
    return draw_pairs(jax.random.fold_in(key, 11), 0.0)[1].astype(jnp.bfloat16)


def draw_q_target(key, part):
    return draw_pairs(jax.random.fold_in(key, 23), 1.0)[0].astype(jnp.bfloat16)


def draw_kv_target(key, part):
    return draw_pairs(jax.random.fold_in(key, 23), 1.0)[1].astype(jnp.bfloat16)


def setup_inputs(seed: int = 0) -> dict:
    key_of = jax.random.split(jax.random.key(seed), 5)
    q_student = draw_q_student(jax.random.fold_in(key_of[4], 71), 0)
    kv_student = draw_kv_student(jax.random.fold_in(key_of[4], 71), 0)
    q_target = draw_q_target(jax.random.fold_in(key_of[4], 71), 0)
    kv_target = draw_kv_target(jax.random.fold_in(key_of[4], 71), 0)
    return dict(q_student=q_student, kv_student=kv_student, q_target=q_target, kv_target=kv_target)


def attend(queries, key_values):
    feature_width = HEADS * HD
    key_all = key_values[:, :feature_width].astype(jnp.float32).reshape(KV_TOKENS, HEADS, HD)
    value_all = key_values[:, feature_width:].astype(jnp.float32).reshape(KV_TOKENS, HEADS, HD)
    blocks = queries.reshape(N_SEQ, TOK_DEV, HEADS, HD)
    score_scale = 1.0 / (HD ** 0.5)

    def one_block(query_block):
        scores = jnp.einsum('qhd,khd->hqk', query_block.astype(jnp.float32), key_all) * score_scale
        row_max = jnp.max(scores, axis=-1, keepdims=True)
        exponent = jnp.exp(scores - row_max)
        row_total = jnp.sum(exponent, axis=-1)
        weights_bf = lax.optimization_barrier(exponent.astype(jnp.bfloat16)).astype(jnp.float32)
        mixed_rows = jnp.einsum('hqk,khd->hqd', weights_bf, value_all) / row_total[:, :, None]
        return jnp.transpose(mixed_rows, (1, 0, 2)).reshape(TOK_DEV, feature_width)

    return lax.map(one_block, blocks).reshape(TOKENS, feature_width)


def reference(q_student, kv_student, q_target, kv_target):
    student_rows = jnp.stack([attend(q_student[clip_index], kv_student[clip_index]) for clip_index in range(CLIPS)])
    target_rows = jnp.stack([attend(q_target[clip_index], kv_target[clip_index]) for clip_index in range(CLIPS)])
    position = jnp.arange(TOKENS).astype(jnp.float32)
    weight = 1.0 + 2.0 * position / float(max(TOKENS - 1, 1))
    gap_rows = student_rows - target_rows
    distill_loss = jnp.sum(weight[None, :, None] * gap_rows * gap_rows) / float(TOKENS * HEADS * HD)
    return student_rows.astype(jnp.bfloat16), target_rows.astype(jnp.bfloat16), distill_loss
```

```python
import functools

import jax
import jax.numpy as jnp
import numpy as np
from jax import lax
from jax.experimental import pallas as pl
from jax.experimental.pallas import tpu as pltpu
from jax.sharding import Mesh
from jax.sharding import PartitionSpec as P

HEADS = 12
HD = 128
HALF = 6
HW = HALF * HD
AXES = ("y", "xl", "z", "c", "dp")
SEQ = AXES[:4]
NY, NX, NZ = 4, 2, 8
VT = HD + 16
SCALE = float(np.log2(np.e) / HD**0.5)


def hop(x, step, first):
    pairs = []
    for y in range(NY):
        for z in range(NZ):
            for c in range(2):
                if (c == 0) == first:
                    y2, z2 = (y + step) % NY, z
                else:
                    y2, z2 = y, (z + step) % NZ
                pairs.append(((y * NZ + z) * 2 + c, (y2 * NZ + z2) * 2 + c))
    return lax.ppermute(x, ("y", "z", "c"), pairs)


def swap_cores(x):
    return lax.ppermute(x, "c", [(0, 1), (1, 0)])


def first_exchange(kv):
    k, v = kv[:, :, : HEADS * HD], kv[:, :, HEADS * HD :]
    halves = [jnp.concatenate([k[:, :, a : a + HW], v[:, :, a : a + HW]], -1) for a in (0, HW)]
    x = jnp.stack(halves * 4, 0)
    groups = [
        [(zz * 2 + xl) * 2 + c for zz in (z, z + 4) for xl in range(2) for c in range(2)] for z in range(4)
    ]
    return lax.all_to_all(
        x, ("z", "xl", "c"), split_axis=0, concat_axis=0, tiled=True, axis_index_groups=groups
    )


def load_kv(refs, k_scr, vt_scr, model):
    at = 0
    for kr, vr in refs:
        n = kr.shape[0] * 8
        k_scr[pl.ds(at, n), :] = kr[:, model].reshape(n, HD)
        vt_scr[pl.ds(0, HD), pl.ds(at, n)] = vr[:, model].reshape(n, HD).T
        at += n
    vt_scr[pl.ds(HD, 16), :] = jnp.ones((16, at), jnp.bfloat16)


def scores_of(k_scr, q):
    return lax.dot_general(k_scr[...], q, (((1,), (1,)), ((), ())), preferred_element_type=jnp.float32)


def weighted(vt_scr, s, m):
    p = jnp.exp2(s * SCALE - m * SCALE).astype(jnp.bfloat16)
    return jnp.dot(vt_scr[...], p, preferred_element_type=jnp.float32)


def kernel_a(nkv, core_ref, qs, qt, qps, qpt, *rest):
    kv, (acc_ref, m_ref, k_scr, vt_scr) = rest[: 2 * nkv], rest[2 * nkv :]
    refs = [(kv[2 * i], kv[2 * i + 1]) for i in range(nkv)]
    rows = qs.shape[0]
    for model, qq in ((0, (qs, qps)), (1, (qt, qpt))):
        load_kv(refs, k_scr.at[model], vt_scr.at[model], model)
    jobs = [(model, w, q) for model, qq in ((0, (qs, qps)), (1, (qt, qpt))) for w, q in enumerate(qq)]
    s = scores_of(k_scr.at[0], jobs[0][2][...])
    for i, (model, w, q) in enumerate(jobs):
        nxt = scores_of(k_scr.at[jobs[i + 1][0]], jobs[i + 1][2][...]) if i < 3 else None
        m = jnp.max(s, axis=0, keepdims=True)
        o = weighted(vt_scr.at[model], s, m)
        acc_ref[0, model, :, pl.ds(w * rows, rows)] = o[: HD + 8]
        m_ref[0, model, :, pl.ds(w * rows, rows)] = m
        s = nxt


def kernel_b(nkv, core_ref, qs, qt, qps, qpt, acc_ref, m_ref, w_ref, *rest):
    kv, (os_ref, ot_ref, op_ref, loss_ref, k_scr, vt_scr, l_scr) = rest[: 2 * nkv], rest[2 * nkv :]
    refs = [(kv[2 * i], kv[2 * i + 1]) for i in range(nkv)]
    rows = qs.shape[0]
    h = pl.program_id(0)
    for model in (0, 1):
        load_kv(refs, k_scr.at[model], vt_scr.at[model], model)
    jobs = [(model, w, q) for w in (0, 1) for model, q in ((0, (qs, qps)[w]), (1, (qt, qpt)[w]))]
    s = scores_of(k_scr.at[0], jobs[0][2][...])
    outs = {}
    for i, (model, w, q) in enumerate(jobs):
        nxt = scores_of(k_scr.at[jobs[i + 1][0]], jobs[i + 1][2][...]) if i < 3 else None
        m_old = m_ref[0, model, :, pl.ds(w * rows, rows)]
        m = jnp.maximum(m_old, jnp.max(s, axis=0, keepdims=True))
        o = weighted(vt_scr.at[model], s, m)
        alpha = jnp.exp2((m_old - m) * SCALE)
        o = acc_ref[0, model, :, pl.ds(w * rows, rows)] * alpha + o[: HD + 8]
        o = o[:HD] / o[HD : HD + 1]
        if w == 0:
            (os_ref, ot_ref)[model][...] = o.T.astype(jnp.bfloat16)
        else:
            op_ref[model] = o.T.astype(jnp.bfloat16)
        outs[model, w] = o
        s = nxt

    @pl.when(h == 0)
    def _():
        l_scr[...] = jnp.zeros_like(l_scr)

    for w in (0, 1):
        d = outs[0, w] - outs[1, w]
        l_scr[:, pl.ds(w * rows, rows)] += jnp.sum(d * d, axis=0, keepdims=True)

    @pl.when(h == HALF - 1)
    def _():
        loss_ref[0] = jnp.sum(l_scr[...] * w_ref[...])


def specs(rows, arrays):
    own = pl.BlockSpec((rows, HD), lambda h, core: (0, core[0] * HALF + h))
    peer = pl.BlockSpec((rows, HD), lambda h, core: (0, h))
    kv = []
    for a in arrays:
        n = a.shape[0]
        kv.append(pl.BlockSpec((n, 2, 8, HD), lambda h, core: (0, 0, 0, h)))
        kv.append(pl.BlockSpec((n, 2, 8, HD), lambda h, core: (0, 0, 0, HALF + h)))
    state = [
        pl.BlockSpec((1, 2, HD + 8, 2 * rows), lambda h, core: (h, 0, 0, 0)),
        pl.BlockSpec((1, 2, 1, 2 * rows), lambda h, core: (h, 0, 0, 0)),
    ]
    return [own, own, peer, peer], kv, state


def params():
    return pltpu.CompilerParams(dimension_semantics=("arbitrary",), vmem_limit_bytes=48 << 20)


def cost(rows, keys):
    n = 4 * rows * keys * HALF
    return pl.CostEstimate(flops=n * HD * 4, bytes_accessed=16 << 20, transcendentals=n)


def attend_a(core, qs, qt, qps, qpt, arrays):
    rows = qs.shape[0]
    keys = sum(a.shape[0] for a in arrays) * 8
    q_specs, kv_specs, state = specs(rows, arrays)
    return pl.pallas_call(
        functools.partial(kernel_a, len(arrays)),
        grid_spec=pltpu.PrefetchScalarGridSpec(
            num_scalar_prefetch=1,
            grid=(HALF,),
            in_specs=q_specs + kv_specs,
            out_specs=state,
            scratch_shapes=[pltpu.VMEM((2, keys, HD), jnp.bfloat16), pltpu.VMEM((2, VT, keys), jnp.bfloat16)],
        ),
        out_shape=[
            jax.ShapeDtypeStruct((HALF, 2, HD + 8, 2 * rows), jnp.float32),
            jax.ShapeDtypeStruct((HALF, 2, 1, 2 * rows), jnp.float32),
        ],
        compiler_params=params(),
        cost_estimate=cost(rows, keys),
        name="attend_a",
    )(core, qs, qt, qps, qpt, *[a for a in arrays for _ in (0, 1)])


def attend_b(core, qs, qt, qps, qpt, acc, m, weight, arrays):
    rows = qs.shape[0]
    keys = sum(a.shape[0] for a in arrays) * 8
    q_specs, kv_specs, state = specs(rows, arrays)
    full = jax.ShapeDtypeStruct((rows, HEADS * HD), jnp.bfloat16)
    return pl.pallas_call(
        functools.partial(kernel_b, len(arrays)),
        grid_spec=pltpu.PrefetchScalarGridSpec(
            num_scalar_prefetch=1,
            grid=(HALF,),
            in_specs=q_specs + state + [pl.BlockSpec((1, 2 * rows), lambda h, core: (0, 0))] + kv_specs,
            out_specs=[
                q_specs[0],
                q_specs[0],
                pl.BlockSpec((2, rows, HD), lambda h, core: (0, 0, h)),
                pl.BlockSpec(memory_space=pltpu.SMEM),
            ],
            scratch_shapes=[
                pltpu.VMEM((2, keys, HD), jnp.bfloat16),
                pltpu.VMEM((2, VT, keys), jnp.bfloat16),
                pltpu.VMEM((1, 2 * rows), jnp.float32),
            ],
        ),
        out_shape=[
            full,
            full,
            jax.ShapeDtypeStruct((2, rows, HW), jnp.bfloat16),
            jax.ShapeDtypeStruct((1,), jnp.float32),
        ],
        compiler_params=params(),
        cost_estimate=cost(rows, keys),
        name="attend_b",
    )(core, qs, qt, qps, qpt, acc, m, weight, *[a for a in arrays for _ in (0, 1)])


def body(q_student, kv_student, q_target, kv_target):
    rows = q_student.shape[1]
    core = lax.axis_index("c")
    qs, qt = q_student[0], q_target[0]

    gathered = first_exchange(jnp.concatenate([kv_student, kv_target], 0))
    q_out = jnp.stack([lax.dynamic_slice_in_dim(q, (1 - core) * HW, HW, 1) for q in (qs, qt)], 0)
    q_in = swap_cores(q_out)
    qps, qpt = q_in[0], q_in[1]
    own = jnp.concatenate([gathered] + [hop(gathered, s, True) for s in (1, -1, 2)], 0)
    lo, hi = own[:16], own[16:]
    lo_up, hi_down = hop(lo, 1, False), hop(hi, -1, False)
    hi_up, lo_down = hop(hi, 1, False), hop(lo, -1, False)
    lo_far, hi_far = hop(lo_up, 1, False), hop(hi_down, -1, False)

    all_tokens = rows * lax.axis_size(SEQ)
    base = lax.axis_index(SEQ) * rows
    other = base + (1 - 2 * core) * rows
    position = jnp.concatenate([base + jnp.arange(rows), other + jnp.arange(rows)]).astype(jnp.float32)
    weight = (1.0 + 2.0 * position / float(max(all_tokens - 1, 1)))[None]

    core1 = core.reshape(1).astype(jnp.int32)
    acc, m = attend_a(core1, qs, qt, qps, qpt, [own, lo_up, hi_down, hi_up, lo_down])
    out_s, out_t, out_p, loss = attend_b(core1, qs, qt, qps, qpt, acc, m, weight, [lo_far, hi_far])
    got = swap_cores(out_p)
    local = loss[0] / float(all_tokens * HEADS * HD)
    for axis in ("c", "xl", "dp", "y", "z"):
        local = lax.psum(local, axis)
    at = (1 - core) * HW
    out_s = lax.dynamic_update_slice(out_s, got[0], (0, at))
    out_t = lax.dynamic_update_slice(out_t, got[1], (0, at))
    return out_s[None], out_t[None], local


def solution(mesh):
    finer = Mesh(mesh.devices.reshape(NY, NX, NZ, 2, mesh.shape["dp"]), AXES)
    spec = P("dp", SEQ, None)
    return jax.shard_map(
        body, mesh=finer, in_specs=(spec,) * 4, out_specs=(spec, spec, P()), check_vma=False
    )
```

```python
import functools

import jax
import jax.numpy as jnp
import numpy as np
from jax import lax
from jax.experimental import pallas as pl
from jax.experimental.pallas import tpu as pltpu
from jax.sharding import Mesh
from jax.sharding import PartitionSpec as P

HEADS = 12
HD = 128
HALF = 6
HW = HALF * HD
AXES = ("y", "xl", "z", "c", "dp")
SEQ = AXES[:4]
NY, NX, NZ = 4, 2, 8
VT = HD + 16
TILE = 256
SCALE = float(np.log2(np.e) / HD**0.5)


def hop(x, step, first):
    pairs = []
    for y in range(NY):
        for z in range(NZ):
            for c in range(2):
                if (c == 0) == first:
                    y2, z2 = (y + step) % NY, z
                else:
                    y2, z2 = y, (z + step) % NZ
                pairs.append(((y * NZ + z) * 2 + c, (y2 * NZ + z2) * 2 + c))
    return lax.ppermute(x, ("y", "z", "c"), pairs)


def swap_cores(x):
    return lax.ppermute(x, "c", [(0, 1), (1, 0)])


def first_exchange(kvs, core):
    def half(c):
        at = (c * HW, HEADS * HD + c * HW)
        return jnp.stack([jnp.concatenate([lax.dynamic_slice_in_dim(kv, a, HW, 1) for a in at], 1) for kv in kvs], 0)

    units = jnp.stack([half(core), swap_cores(half(1 - core))], 0)
    units = jnp.concatenate([units, lax.ppermute(units, "z", [(i, (i + 4) % NZ) for i in range(NZ)])], 0)
    return jnp.concatenate([units, lax.ppermute(units, "xl", [(0, 1), (1, 0)])], 0)


def kernel(first, last, nkv, core_ref, *refs):
    refs = list(refs)
    take = lambda n: [refs.pop(0) for _ in range(n)]
    queries = take(4)
    acc_in, m_in = (None, None) if first else take(2)
    w_ref = take(1)[0] if last else None
    kv = take(2 * nkv)
    outs = take(4) if last else take(2)
    sets = [take(3), take(3)]
    rows = queries[0].shape[0]
    keys = sets[0][1].shape[2]
    per = rows // TILE
    g = pl.program_id(0)
    jobs = [(t, model) for t in range(2 * per) for model in (0, 1)]
    if last:
        l_scr = refs[0]

        @pl.when(g <= 1)
        def _():
            l_scr[...] = jnp.zeros_like(l_scr)

    def both(new, old):
        s_new, vt_new, m_new = new
        s_old, vt_old, m_old_ref = old
        ks = []
        for model in (0, 1):
            ks.append(jnp.concatenate([kv[2 * i][:, model].reshape(-1, HD) for i in range(nkv)], 0))
            at = 0
            for i in range(nkv):
                n = kv[2 * i].shape[0] * 8
                vt_new[model, pl.ds(0, HD), pl.ds(at, n)] = kv[2 * i + 1][:, model].reshape(n, HD).T
                at += n
            vt_new[model, pl.ds(HD, 16), :] = jnp.ones((16, keys), jnp.bfloat16)
        done = {}
        for i, (t, model) in enumerate(jobs):
            cols = pl.ds(t * TILE, TILE)
            r = pl.ds((t % per) * TILE, TILE)
            s = lax.dot_general(
                ks[model],
                queries[2 * (t // per) + model][r, :],
                (((1,), (1,)), ((), ())),
                preferred_element_type=jnp.float32,
            )
            s_new[i] = s
            m_new[i] = jnp.max(s, axis=0, keepdims=True)

            m = m_old_ref[i]
            if not first:
                before = m_in[0, model, :, cols]
                m = jnp.maximum(before, m)
            shift = m * SCALE
            o = None
            for k in range(0, keys, TILE):
                p = jnp.exp2(s_old[i, pl.ds(k, TILE), :] * SCALE - shift).astype(jnp.bfloat16)
                d = jnp.dot(vt_old[model, :, pl.ds(k, TILE)], p, preferred_element_type=jnp.float32)
                o = d if o is None else o + d
            o = o[: HD + 8]
            if not first:
                o = acc_in[0, model, :, cols] * jnp.exp2(before * SCALE - shift) + o
            if not last:
                outs[0][0, model, :, cols] = o
                outs[1][0, model, :, cols] = m
                continue
            o = o[:HD] * (1.0 / o[HD : HD + 1])
            ob = o.astype(jnp.bfloat16).T
            if t < per:
                outs[model][r, :] = ob
            else:
                outs[2][model, r, :] = ob
            if model == 0:
                done[t] = o
            else:
                e = done.pop(t) - o
                l_scr[:, cols] += jnp.sum(e * e, axis=0, keepdims=True)

    @pl.when(g % 2 == 0)
    def _():
        both(sets[0], sets[1])

    @pl.when(g % 2 == 1)
    def _():
        both(sets[1], sets[0])

    if last:

        @pl.when(g == HALF)
        def _():
            outs[3][...] = jnp.full((1, HD), jnp.sum(l_scr[...] * w_ref[...]), jnp.float32)


def attend(core, queries, arrays, state=None, weight=None):
    rows = queries[0].shape[0]
    first, last = state is None, weight is not None
    keys = sum(a.shape[0] for a in arrays) * 8
    now = lambda g: jnp.minimum(g, HALF - 1)
    past = lambda g: jnp.maximum(g - 1, 0)
    own = pl.BlockSpec((rows, HD), lambda g, core: (0, core[0] * HALF + now(g)))
    state_specs = [
        pl.BlockSpec((1, 2, HD + 8, 2 * rows), lambda g, core: (past(g), 0, 0, 0)),
        pl.BlockSpec((1, 2, 1, 2 * rows), lambda g, core: (past(g), 0, 0, 0)),
    ]
    in_specs, args = [own] * 4, list(queries)
    if not first:
        in_specs += state_specs
        args += [pltpu.with_memory_space_constraint(state[0], pltpu.HBM), state[1]]
    if last:
        in_specs.append(pl.BlockSpec((1, 2 * rows), lambda g, core: (0, 0)))
        args.append(weight)
    for a in arrays:
        for base in (0, HALF):
            in_specs.append(pl.BlockSpec((a.shape[0], 2, 8, HD), lambda g, core, base=base: (0, 0, 0, base + now(g))))
            args.append(a)
    jobs = 4 * rows // TILE
    scratch = [
        pltpu.VMEM((jobs, keys, TILE), jnp.float32),
        pltpu.VMEM((2, VT, keys), jnp.bfloat16),
        pltpu.VMEM((jobs, 1, TILE), jnp.float32),
    ] * 2
    if last:
        full = jax.ShapeDtypeStruct((rows, HEADS * HD), jnp.bfloat16)
        out = pl.BlockSpec((rows, HD), lambda g, core: (0, core[0] * HALF + past(g)))
        out_specs = [out, out, pl.BlockSpec((2, rows, HD), lambda g, core: (0, 0, past(g))), pl.BlockSpec((1, HD), lambda g, core: (0, 0))]
        out_shape = [full, full, jax.ShapeDtypeStruct((2, rows, HW), jnp.bfloat16), jax.ShapeDtypeStruct((1, HD), jnp.float32)]
        scratch.append(pltpu.VMEM((1, 2 * rows), jnp.float32))
    else:
        out_specs = state_specs
        out_shape = [
            pltpu.HBM((HALF, 2, HD + 8, 2 * rows), jnp.float32),
            jax.ShapeDtypeStruct((HALF, 2, 1, 2 * rows), jnp.float32),
        ]
    n = 4 * rows * keys * HALF
    return pl.pallas_call(
        functools.partial(kernel, first, last, len(arrays)),
        grid_spec=pltpu.PrefetchScalarGridSpec(
            num_scalar_prefetch=1, grid=(HALF + 1,), in_specs=in_specs, out_specs=out_specs, scratch_shapes=scratch
        ),
        out_shape=out_shape,
        compiler_params=pltpu.CompilerParams(dimension_semantics=("arbitrary",), vmem_limit_bytes=(14 if last else 12 if first else 18) << 20),
        cost_estimate=pl.CostEstimate(flops=n * HD * 4, bytes_accessed=16 << 20, transcendentals=n),
        name="attend_last" if last else "attend_first" if first else "attend_next",
    )(core, *args)


def body(q_student, kv_student, q_target, kv_target):
    rows = q_student.shape[1]
    core = lax.axis_index("c")
    qs, qt = q_student[0], q_target[0]

    units = first_exchange((kv_student[0], kv_target[0]), core)
    qs_x, qt_x, _ = lax.optimization_barrier((qs, qt, units[0, 0, :, :HD]))
    queries = [qs, qt, swap_cores(qs_x), swap_cores(qt_x)]
    lo = jnp.concatenate([units, hop(units, 1, True)], 0)
    hi = jnp.concatenate([hop(units, -1, True), hop(units, 2, True)], 0)
    lo_up, hi_down = hop(lo, 1, False), hop(hi, -1, False)
    hi_up, lo_down = hop(hi, 1, False), hop(lo, -1, False)

    all_tokens = rows * lax.axis_size(SEQ)
    base = lax.axis_index(SEQ) * rows
    other = base + (1 - 2 * core) * rows
    position = jnp.concatenate([base + jnp.arange(rows), other + jnp.arange(rows)]).astype(jnp.float32)
    weight = (1.0 + 2.0 * position / float(max(all_tokens - 1, 1)))[None]

    core1 = core.reshape(1).astype(jnp.int32)
    state = attend(core1, queries, [lo, hi])
    lo_up_x, hi_down_x, _ = lax.optimization_barrier((lo_up, hi_down, state[1]))
    lo_far, hi_far = hop(lo_up_x, 1, False), hop(hi_down_x, -1, False)
    state = attend(core1, queries, [lo_up, hi_down, hi_up, lo_down], state)
    out_s, out_t, out_p, loss = attend(core1, queries, [lo_far, hi_far], state, weight)
    got = swap_cores(out_p)
    loss = over_devices(loss) / float(all_tokens * HEADS * HD)
    at = (1 - core) * HW
    out_s = lax.dynamic_update_slice(out_s, got[0], (0, at))
    out_t = lax.dynamic_update_slice(out_t, got[1], (0, at))
    return out_s[None], out_t[None], loss


def over_devices(x):
    n = 2 * NY * NX * NZ * lax.axis_size("dp")
    every = lax.all_to_all(
        jnp.broadcast_to(x, (n, 1, HD)), AXES, split_axis=0, concat_axis=0, tiled=True
    )
    return jnp.sum(every) / HD


def solution(mesh):
    finer = Mesh(mesh.devices.reshape(NY, NX, NZ, 2, mesh.shape["dp"]), AXES)
    spec = P("dp", SEQ, None)
    return jax.shard_map(
        body, mesh=finer, in_specs=(spec,) * 4, out_specs=(spec, spec, P()), check_vma=False
    )
```

```python
import functools

import jax
import jax.numpy as jnp
import numpy as np
from jax import lax
from jax.experimental import pallas as pl
from jax.experimental.pallas import tpu as pltpu
from jax.sharding import Mesh
from jax.sharding import PartitionSpec as P

HEADS = 12
HD = 128
HALF = 6
HW = HALF * HD
AXES = ("y", "xl", "z", "c", "dp")
SEQ = AXES[:4]
NY, NX, NZ = 4, 2, 8
VT = HD + 16
TILE = 256
MROW = HD + 4
SCALE = float(np.log2(np.e) / HD**0.5)


def hop(x, step, first):
    pairs = []
    for y in range(NY):
        for z in range(NZ):
            for c in range(2):
                if (c == 0) == first:
                    y2, z2 = (y + step) % NY, z
                else:
                    y2, z2 = y, (z + step) % NZ
                pairs.append(((y * NZ + z) * 2 + c, (y2 * NZ + z2) * 2 + c))
    return lax.ppermute(x, ("y", "z", "c"), pairs)


def swap_cores(x):
    return lax.ppermute(x, "c", [(0, 1), (1, 0)])


def far_z(x):
    return lax.ppermute(x, "z", [(i, (i + 4) % NZ) for i in range(NZ)])


def swap_x(x):
    return lax.ppermute(x, "xl", [(0, 1), (1, 0)])


def first_exchange(kvs, core):
    def half(c):
        at = (c * HW, HEADS * HD + c * HW)
        return jnp.stack([jnp.concatenate([lax.dynamic_slice_in_dim(kv, a, HW, 1) for a in at], 1) for kv in kvs], 0)

    units = jnp.stack([half(core), swap_cores(half(1 - core))], 0)
    units = jnp.concatenate([units, far_z(units)], 0)
    return jnp.concatenate([units, swap_x(units)], 0)


def kernel(first, last, units, *refs):
    refs = list(refs)
    take = lambda n: [refs.pop(0) for _ in range(n)]
    nkv = len(units)
    queries = take(4)
    acc_in = None if first else take(1)[0]
    w_ref = take(1)[0] if last else None
    kv = take(nkv)
    outs = take(4) if last else take(1)
    sets = [take(3), take(3)]
    l_scr = take(1)[0] if last else None
    if first:
        state_out, state_sem = outs[0], refs[1]
        outs = [refs[0]]
    elif not last:
        state_in, state_sem = acc_in, refs[1]
        acc_in = refs[0]
        for h in range(HALF):
            pltpu.make_async_copy(state_in.at[h], acc_in.at[h], state_sem.at[h]).start()
    core = lax.axis_index("c")
    rows = queries[0].shape[0]
    keys = sum(units) * 8
    per = rows // TILE
    jobs = [(t, model) for t in range(2 * per) for model in (0, 1)]
    if last:
        l_scr[...] = jnp.zeros_like(l_scr)

    def work(g, new, old):
        if new is not None:
            s_new, vt_new, m_new = new
            kc = pl.ds(pl.multiple_of(g * HD, HD), HD)
            vc = pl.ds(pl.multiple_of(HW + g * HD, HD), HD)
            qc = pl.ds(pl.multiple_of(core * HW + g * HD, HD), HD)
            ks = [jnp.concatenate([a[:, model, :, kc].reshape(-1, HD) for a in kv], 0) for model in (0, 1)]
            for model in (0, 1):
                at = 0
                for a, n in zip(kv, units):
                    vt_new[model, pl.ds(0, HD), pl.ds(at, n * 8)] = a[:, model, :, vc].reshape(n * 8, HD).T
                    at += n * 8
                vt_new[model, pl.ds(HD, 16), :] = jnp.ones((16, keys), jnp.bfloat16)
        if old is not None:
            s_old, vt_old, m_old = old
            mine = pl.ds(pl.multiple_of(core * HW + (g - 1) * HD, HD), HD)
            sent = pl.ds(pl.multiple_of((g - 1) * HD, HD), HD)
            if not first and not last:
                pltpu.make_async_copy(state_in.at[g - 1], acc_in.at[g - 1], state_sem.at[g - 1]).wait()
        done = {}
        for i, (t, model) in enumerate(jobs):
            cols = pl.ds(t * TILE, TILE)
            r = pl.ds((t % per) * TILE, TILE)
            if new is not None:
                s = lax.dot_general(
                    ks[model],
                    queries[2 * (t // per) + model][r, qc],
                    (((1,), (1,)), ((), ())),
                    preferred_element_type=jnp.float32,
                )
                s_new[i] = s
                m_new[i] = jnp.max(s, axis=0, keepdims=True)
            if old is None:
                continue
            m = m_old[i]
            if not first:
                before = acc_in[g - 1, model, pl.ds(MROW, 1), cols]
                m = jnp.maximum(before, m)
            shift = m * SCALE
            o = None
            for k in range(0, keys, TILE):
                p = jnp.exp2(s_old[i, pl.ds(k, TILE), :] * SCALE - shift).astype(jnp.bfloat16)
                d = jnp.dot(vt_old[model, :, pl.ds(k, TILE)], p, preferred_element_type=jnp.float32)
                o = d if o is None else o + d
            o = o[: HD + 8]
            if not first:
                o = acc_in[g - 1, model, :, cols] * jnp.exp2(before * SCALE - shift) + o
            if not last:
                outs[0][g - 1, model, :, cols] = o
                outs[0][g - 1, model, pl.ds(MROW, 1), cols] = m
                continue
            o = o[:HD] * (1.0 / o[HD : HD + 1])
            ob = o.astype(jnp.bfloat16).T
            if t < per:
                outs[model][r, mine] = ob
            else:
                outs[2][model, r, sent] = ob
            if model == 0:
                done[t] = o
            else:
                e = done.pop(t) - o
                l_scr[:, cols] += jnp.sum(e * e, axis=0, keepdims=True)
        if first and old is not None:
            pltpu.make_async_copy(outs[0].at[g - 1], state_out.at[g - 1], state_sem.at[g - 1]).start()

    work(0, sets[0], None)

    def two(j, carry):
        work(2 * j + 1, sets[1], sets[0])
        work(2 * j + 2, sets[0], sets[1])
        return carry

    lax.fori_loop(0, (HALF - 1) // 2, two, 0)
    work(HALF - 1, sets[1], sets[0])
    work(HALF, None, sets[1])
    if first:
        for h in range(HALF):
            pltpu.make_async_copy(outs[0].at[h], state_out.at[h], state_sem.at[h]).wait()
    if last:
        outs[3][...] = jnp.full(outs[3].shape, jnp.sum(l_scr[...] * w_ref[...]), jnp.float32)


def attend(queries, arrays, state=None, weight=None):
    rows = queries[0].shape[0]
    first, last = state is None, weight is not None
    units = [a.shape[0] for a in arrays]
    keys = sum(units) * 8
    args = list(queries) + ([] if first else [state]) + ([weight] if last else []) + arrays
    here, anywhere = pl.BlockSpec(memory_space=pltpu.VMEM), pl.BlockSpec(memory_space=pl.ANY)
    in_specs = [here] * len(args)
    through = not first and not last
    if through:
        in_specs[4] = anywhere
    args = [a if s is anywhere or (first and i < 4) else pltpu.with_memory_space_constraint(a, pltpu.VMEM) for i, (a, s) in enumerate(zip(args, in_specs))]
    jobs = 4 * rows // TILE
    scratch = [
        pltpu.VMEM((jobs, keys, TILE), jnp.float32),
        pltpu.VMEM((2, VT, keys), jnp.bfloat16),
        pltpu.VMEM((jobs, 1, TILE), jnp.float32),
    ] * 2
    if last:
        scratch.append(pltpu.VMEM((1, 2 * rows), jnp.float32))
        full = pltpu.VMEM((rows, HEADS * HD), jnp.bfloat16)
        out_shape = [
            full,
            full,
            pltpu.HBM((2, rows, HW), jnp.bfloat16),
            pltpu.VMEM((lax.axis_size(AXES), 1, HD), jnp.float32),
        ]
    else:
        out_shape = [(pltpu.HBM if first else pltpu.VMEM)((HALF, 2, HD + 8, 2 * rows), jnp.float32)]
    if not last:
        scratch += [pltpu.VMEM((HALF, 2, HD + 8, 2 * rows), jnp.float32), pltpu.SemaphoreType.DMA((HALF,))]
    n = 4 * rows * keys * HALF
    return pl.pallas_call(
        functools.partial(kernel, first, last, units),
        in_specs=in_specs,
        out_specs=[anywhere if first else here] * len(out_shape),
        scratch_shapes=scratch,
        out_shape=out_shape,
        compiler_params=pltpu.CompilerParams(vmem_limit_bytes=(20 if last else 24 if first else 34) << 20),
        cost_estimate=pl.CostEstimate(flops=n * HD * 4, bytes_accessed=16 << 20, transcendentals=n),
        name="attend_last" if last else "attend_first" if first else "attend_next",
    )(*args)


def layer(q_student, kv_student, q_target, kv_target):
    rows = q_student.shape[1]
    core = lax.axis_index("c")
    qs, qt = q_student[0], q_target[0]

    units = first_exchange((kv_student[0], kv_target[0]), core)
    queries = [qs, qt, swap_cores(qs), swap_cores(qt)]
    lo = jnp.concatenate([units, hop(units, 1, True)], 0)
    hi = jnp.concatenate([hop(units, -1, True), hop(units, 2, True)], 0)
    lo_up, lo_down = hop(lo, 1, False), hop(lo, -1, False)
    hi_up, hi_down = hop(hi, 1, False), hop(hi, -1, False)
    lo_far, hi_far = hop(lo_up, 1, False), hop(hi_down, -1, False)

    all_tokens = rows * lax.axis_size(SEQ)
    base = lax.axis_index(SEQ) * rows
    other = base + (1 - 2 * core) * rows
    position = jnp.concatenate([base + jnp.arange(rows), other + jnp.arange(rows)]).astype(jnp.float32)
    weight = (1.0 + 2.0 * position / float(max(all_tokens - 1, 1)))[None]

    (state,) = attend(queries, [lo, hi])
    (state,) = attend(queries, [lo_up, lo_down, hi_up, hi_down], state)
    out_s, out_t, out_p, loss = attend(queries, [lo_far, hi_far], state, weight)
    loss = over_devices(loss) / float(all_tokens * HEADS * HD)
    got = swap_cores(out_p)
    at = (1 - core) * HW
    out_s = lax.dynamic_update_slice(out_s, got[0], (0, at))
    out_t = lax.dynamic_update_slice(out_t, got[1], (0, at))
    return out_s[None], out_t[None], loss


def over_devices(x):
    return jnp.sum(lax.all_to_all(x, AXES, split_axis=0, concat_axis=0, tiled=True)) / HD


def solution(mesh):
    finer = Mesh(mesh.devices.reshape(NY, NX, NZ, 2, mesh.shape["dp"]), AXES)
    spec = P("dp", SEQ, None)
    return jax.shard_map(layer, mesh=finer, in_specs=(spec,) * 4, out_specs=(spec, spec, P()), check_vma=False)
```
